8 devices in a mesh: dp: 1 (over z), m3: 2 (over y), m2: 2 (over x), m1: 2 (over core).
Axes of the slice: x: 2, y: 2, z: 1, core: 2. Of those that a mesh axis runs over, the one named last changes fastest.
Arguments:
- volume: bfloat16 [128, 128, 128, 128], P('dp', 'm1', 'm2', 'm3')
- fac_one: bfloat16 [128, 128], replicated
- fac_two: bfloat16 [128, 128], replicated
- fac_three: bfloat16 [128, 128], replicated
- diag_scale: float32 [128, 128, 128], P('m2', 'm1')
Outputs:
- output: bfloat16 [128, 128, 128, 128], P(('dp', 'm3'), 'm2', 'm1')
All inputs are finite; a program needn't handle non-finite values.
Results may differ from the reference program's by a relative error of at most 0.00844248.
Values are sent between devices in bfloat16 or wider.
A program may use at most 1 GiB of HBM per device.

```python
import jax
import jax.numpy as jnp
from jax import lax

GRID_ONE = 128
GRID_TWO = 128
GRID_THREE = 128
RHS_PART = 128


def orthonormal(rng_key, mat_order):
    gaussian = jax.random.normal(rng_key, (mat_order, mat_order), jnp.float32)
    ortho_mat = jnp.linalg.qr(gaussian)[0]
    return ortho_mat.astype(jnp.bfloat16)


def setup_inputs(seed: int = 0, part: int = 0) -> dict:
    base_key = jax.random.key(seed)
    key_list = jax.random.split(base_key, 5)
    vol_key = jax.random.fold_in(key_list[0], part)
    volume = jax.random.normal(vol_key, (RHS_PART, GRID_ONE, GRID_TWO, GRID_THREE), jnp.float32).astype(jnp.bfloat16)
    fac_one = orthonormal(key_list[1], GRID_ONE)
    fac_two = orthonormal(key_list[2], GRID_TWO)
    fac_three = orthonormal(key_list[3], GRID_THREE)
    log_diag = jax.random.uniform(key_list[4], (GRID_THREE, GRID_TWO, GRID_ONE), jnp.float32, -1.15, 1.15)
    diag_scale = jnp.exp(log_diag)
    return {"volume": volume, "fac_one": fac_one, "fac_two": fac_two, "fac_three": fac_three, "diag_scale": diag_scale}


def reference(volume, fac_one, fac_two, fac_three, diag_scale):
    one_wide = fac_one.astype(jnp.float32)
    two_wide = fac_two.astype(jnp.float32)
    three_wide = fac_three.astype(jnp.float32)

    def per_rhs(vol_one):
        prod_three = jnp.einsum("abl,kl->abk", vol_one.astype(jnp.float32), three_wide).astype(jnp.bfloat16)
        prod_two = jnp.einsum("abk,jb->akj", prod_three.astype(jnp.float32), two_wide).astype(jnp.bfloat16)
        prod_one = jnp.einsum("akj,ia->kji", prod_two.astype(jnp.float32), one_wide).astype(jnp.bfloat16)
        return (diag_scale * prod_one.astype(jnp.float32)).astype(jnp.bfloat16)

    return lax.map(per_rhs, volume)
```

```python
import functools

import jax
import jax.numpy as jnp
from jax import lax
from jax.experimental import pallas as pl
from jax.experimental.pallas import tpu as pltpu
from jax.sharding import PartitionSpec as P

MESH = pl.DeviceIdType.MESH
BF16, F32 = jnp.bfloat16, jnp.float32
UNITS = 128
AHEAD = 4
LAG = 6
PITCH = 24


def exchange_kernel(x_hbm, a3_ref, a2_ref, z_hbm, xbuf, pk, yr, xs, vo, vr, t3, t2, zo, zs,
                    x_sem, ys_sem, yr_sem, xs_sem, xr_sem, zl_sem, zs_sem, zr_sem, y_free, x_free, z_free):
    y, x, c = lax.axis_index("m3"), lax.axis_index("m2"), lax.axis_index("m1")

    barrier = pltpu.get_barrier_semaphore()
    for peer in ({"m3": 1 - y}, {"m2": 1 - x}, {"m1": 1 - c}):
        pl.semaphore_signal(barrier, inc=1, device_id=peer, device_id_type=MESH)
    pl.semaphore_wait(barrier, 3)

    def load(r):
        return pltpu.make_async_copy(
            x_hbm.at[pl.ds((r // 16) * 8, 8), pl.ds((r % 16) * 4, 4)], xbuf.at[r % 4], x_sem.at[r % 4])

    def pack(r):
        slot, part, quarter, pair = r % 4, (r // 16) % 2, (r // 4) % 4, (r % 4) * 2
        for a in range(8):
            for j in range(2):
                tile = xbuf[slot, a, 2 * j:2 * j + 2].reshape(128, 128).T
                for block in range(8):
                    pk[part, block // 4, block % 4, quarter, pair + j, a * 16:(a + 1) * 16, :] = (
                        tile[block * 16:(block + 1) * 16, :])

    def send_y(u):
        return pltpu.make_async_remote_copy(
            src_ref=pk.at[(u // 16) % 2, 1 - y, (u // 4) % 4, u % 4], dst_ref=yr.at[u % 8],
            send_sem=ys_sem.at[u % 8], recv_sem=yr_sem.at[u % 8], device_id={"m3": 1 - y}, device_id_type=MESH)

    def send_x(u):
        return pltpu.make_async_remote_copy(
            src_ref=xs.at[u % 4], dst_ref=vr.at[(u // 4) % 4, u % 4],
            send_sem=xs_sem.at[u % 4], recv_sem=xr_sem.at[(u // 4) % 4, u % 4],
            device_id={"m2": 1 - x}, device_id_type=MESH)

    def z_place(v):
        return z_hbm.at[pl.ds(((v // 4) % 4) * 16, 16), pl.ds((v % 4) * 8, 8), pl.ds(c * 64 + (v // 16) * 8, 8)]

    def keep_z(v):
        return pltpu.make_async_copy(zo.at[v % 4], z_place(v), zl_sem.at[v % 4])

    def send_z(v):
        return pltpu.make_async_remote_copy(
            src_ref=zs.at[v % 4], dst_ref=z_place(v), send_sem=zs_sem.at[v % 4], recv_sem=zr_sem.at[v % 4],
            device_id={"m1": 1 - c}, device_id_type=MESH)

    def product_three(u):
        part, group, quarter, slot = (u // 16) % 2, (u // 4) % 4, u % 4, u % 8
        chunk = (u // 4) % 4
        for pair in range(4):
            rows = []
            for j in range(2):
                own = pk[part, y, group, quarter, 2 * pair + j]
                other = yr[slot, 2 * pair + j]
                rows.append(jnp.concatenate([own, other], axis=1))
            prod = lax.dot_general(a3_ref[...], jnp.concatenate(rows, axis=0), (((1,), (1,)), ((), ())),
                                   preferred_element_type=F32)
            for j in range(2):
                for b in range(2):
                    t3[pl.ds((2 * pair + j) * 2 + b, 128, stride=PITCH), :] = (
                        prod[b * 128:(b + 1) * 128, j * 128:(j + 1) * 128])
        for k in range(64):
            vo[chunk, quarter, k] = t3[k * PITCH:k * PITCH + 16, :].astype(BF16)
        for k in range(64):
            xs[u % 4, k] = t3[(64 + k) * PITCH:(64 + k) * PITCH + 16, :].astype(BF16)

    def product_two(v):
        chunk, quarter, slot = (v // 4) % 4, v % 4, v % 4

        def pair(kk, carry):
            cols = []
            for j in range(2):
                k = (quarter * 8 + kk) * 2 + j
                cols.append(jnp.concatenate([vo[chunk, q, k] for q in range(4)] + [vr[chunk, q, k] for q in range(4)],
                                            axis=0))
            prod = jnp.dot(a2_ref[...], jnp.concatenate(cols, axis=1), preferred_element_type=F32)
            for h, out in enumerate((zo, zs)):
                turned = jnp.concatenate(
                    [prod[h * 64:(h + 1) * 64, :128], prod[h * 64:(h + 1) * 64, 128:]], axis=0).T
                for t in range(16):
                    t2[h, pl.ds((t % 2) * 64 + t // 2, 8, stride=8), :] = turned[t * 8:(t + 1) * 8, :]
                for s in range(16):
                    out[slot, s, kk] = t2[h, s * 8:(s + 1) * 8, :].astype(BF16)
            return carry

        lax.fori_loop(0, 8, pair, 0)

    for r in range(3):
        load(r).start()

    def prologue(r, carry):
        load(r).wait()
        load(r + 3).start()
        pack(r)

        @pl.when(r % 4 == 3)
        def _():
            send_y(r // 4).start()

        return carry

    lax.fori_loop(0, 16, prologue, 0)

    def step(m, carry):
        @pl.when(m < UNITS)
        def _():
            send_y(m).wait_recv()

            @pl.when(m >= 4)
            def _():
                send_x(m - 4).wait_send()

            product_three(m)
            send_y(m).wait_send()

            @pl.when(m < UNITS - 8)
            def _():
                pl.semaphore_signal(y_free, inc=1, device_id={"m3": 1 - y}, device_id_type=MESH)

        @pl.when(m < UNITS - 16)
        def _():
            r = m + 16
            load(r).wait()

            @pl.when(r < UNITS - 3)
            def _():
                load(r + 3).start()

            pack(r)

        @pl.when(m < UNITS - AHEAD)
        def _():
            @pl.when(m >= 4)
            def _():
                pl.semaphore_wait(y_free, 1)

            send_y(m + AHEAD).start()

        @pl.when(m < UNITS)
        def _():
            @pl.when((m % 4 == 0) & (m >= 16))
            def _():
                pl.semaphore_wait(x_free, 1)

            send_x(m).start()

        @pl.when(m >= LAG)
        def _():
            v = m - LAG

            @pl.when(v % 4 == 0)
            def _():
                for q in range(4):
                    send_x(v + q).wait_recv()

            @pl.when(v >= 4)
            def _():
                keep_z(v - 4).wait()
                send_z(v - 4).wait_send()
                pl.semaphore_wait(z_free, 1)

            product_two(v)

            @pl.when((v % 4 == 3) & (v < UNITS - 16))
            def _():
                pl.semaphore_signal(x_free, inc=1, device_id={"m2": 1 - x}, device_id_type=MESH)

            keep_z(v).start()
            send_z(v).start()

            @pl.when(v >= 2)
            def _():
                send_z(v - 2).wait_recv()

                @pl.when(v < UNITS - 2)
                def _():
                    pl.semaphore_signal(z_free, inc=1, device_id={"m1": 1 - c}, device_id_type=MESH)

        return carry

    lax.fori_loop(0, UNITS + LAG, step, 0)

    for u in range(UNITS - 4, UNITS):
        send_x(u).wait_send()
        keep_z(u).wait()
        send_z(u).wait_send()
    for u in range(UNITS - 2, UNITS):
        send_z(u).wait_recv()


def exchange(xt, a3, a2):
    flops = 2 * (512 * 256 * 256 * 256 + 32 * 64 * 128 * 128 * 128)
    return pl.pallas_call(
        exchange_kernel,
        name="exchange",
        out_shape=jax.ShapeDtypeStruct((64, 32, 128, 128), BF16),
        in_specs=[pl.BlockSpec(memory_space=pl.ANY), pl.BlockSpec(memory_space=pltpu.VMEM),
                  pl.BlockSpec(memory_space=pltpu.VMEM)],
        out_specs=pl.BlockSpec(memory_space=pl.ANY),
        scratch_shapes=[
            pltpu.VMEM((4, 8, 4, 64, 128), BF16),
            pltpu.VMEM((2, 2, 4, 4, 8, 128, 128), BF16),
            pltpu.VMEM((8, 8, 128, 128), BF16),
            pltpu.VMEM((4, 64, 16, 128), BF16),
            pltpu.VMEM((4, 4, 64, 16, 128), BF16),
            pltpu.VMEM((4, 4, 64, 16, 128), BF16),
            pltpu.VMEM((128 * PITCH, 128), F32),
            pltpu.VMEM((2, 128, 128), F32),
            pltpu.VMEM((4, 16, 8, 8, 128), BF16),
            pltpu.VMEM((4, 16, 8, 8, 128), BF16),
            pltpu.SemaphoreType.DMA((4,)),
            pltpu.SemaphoreType.DMA((8,)),
            pltpu.SemaphoreType.DMA((8,)),
            pltpu.SemaphoreType.DMA((4,)),
            pltpu.SemaphoreType.DMA((4, 4)),
            pltpu.SemaphoreType.DMA((4,)),
            pltpu.SemaphoreType.DMA((4,)),
            pltpu.SemaphoreType.DMA((4,)),
            pltpu.SemaphoreType.REGULAR,
            pltpu.SemaphoreType.REGULAR,
            pltpu.SemaphoreType.REGULAR,
        ],
        cost_estimate=pl.CostEstimate(flops=flops, bytes_accessed=2 * 64 * 2**20, transcendentals=0),
        compiler_params=pltpu.CompilerParams(collective_id=0, has_side_effects=True, vmem_limit_bytes=62 * 2**20),
    )(xt, a3, a2)


def last_kernel(z_ref, a1_ref, d_ref, w_ref):
    for kk in range(32):
        prod = lax.dot_general(z_ref[0, kk], a1_ref[...], (((0,), (1,)), ((), ())), preferred_element_type=F32)
        scale = d_ref[2 * kk:2 * kk + 2].reshape(128, 128)
        w_ref[0, 2 * kk:2 * kk + 2] = (scale * prod.astype(BF16).astype(F32)).astype(BF16).reshape(2, 64, 128)


def last_product(z, a1, d):
    return pl.pallas_call(
        last_kernel,
        name="last_product",
        grid=(64,),
        out_shape=jax.ShapeDtypeStruct((64, 64, 64, 128), BF16),
        in_specs=[pl.BlockSpec((1, 32, 128, 128), lambda s: (s, 0, 0, 0)), pl.BlockSpec((128, 128), lambda s: (0, 0)),
                  pl.BlockSpec((64, 64, 128), lambda s: (0, 0, 0))],
        out_specs=pl.BlockSpec((1, 64, 64, 128), lambda s: (s, 0, 0, 0)),
        cost_estimate=pl.CostEstimate(flops=2 * 64 * 4096 * 128 * 128, bytes_accessed=2 * 64 * 2**20, transcendentals=0),
        compiler_params=pltpu.CompilerParams(vmem_limit_bytes=32 * 2**20),
    )(z, a1, d)


def solution(mesh):
    def local_step(vol_blk, fac_one, fac_two, fac_three, diag_blk):
        y, x, c = lax.axis_index("m3"), lax.axis_index("m2"), lax.axis_index("m1")

        def own_first(mat, index, axis):
            return jnp.where(index == 0, mat, jnp.roll(mat, 64, axis))

        three = own_first(own_first(fac_three, x, 0), y, 1)
        three = jnp.einsum("bc,ksl->bkscl", jnp.eye(2, dtype=BF16), three.reshape(128, 2, 64)).reshape(256, 256)
        two = own_first(own_first(fac_two, c, 0), x, 1)
        z = exchange(jnp.transpose(vol_blk, (1, 2, 3, 0)), three, two)
        return last_product(z, fac_one, diag_blk)

    return jax.shard_map(local_step, mesh=mesh, in_specs=(P("dp", "m1", "m2", "m3"), P(), P(), P(), P("m2", "m1", None)),
                         out_specs=P(("dp", "m3"), "m2", "m1", None), check_vma=False)
```
